32 devices in a mesh: dp: 1, tp: 32 (over x, y, z, core).
Axes of the slice: x: 2, y: 2, z: 4, core: 2. Of those that a mesh axis runs over, the one named last changes fastest.
Arguments:
- x: bfloat16 [2048, 5120], P('dp')
- dy: bfloat16 [2048, 5120], P('dp')
- gate: bfloat16 [2048, 32768], P('dp', 'tp')
- up: bfloat16 [2048, 32768], P('dp', 'tp')
- w_gate: bfloat16 [5120, 32768], P(None, 'tp')
- w_up: bfloat16 [5120, 32768], P(None, 'tp')
- w_down: bfloat16 [32768, 5120], P('tp')
Outputs:
- output 1: bfloat16 [2048, 5120], P('dp')
- output 2: bfloat16 [5120, 32768], P('dp', 'tp')
- output 3: bfloat16 [5120, 32768], P('dp', 'tp')
- output 4: bfloat16 [32768, 5120], P(('dp', 'tp'))
All inputs are finite; a program needn't handle non-finite values.
Results may differ from the reference program's by a relative error of at most 0.012.
Values are sent between devices in bfloat16 or wider.
A program may use at most 2 GiB of HBM per device.

```python
import jax
import jax.numpy as jnp

ROWS = 2048
D = 5120
FF = 32768


def act(gate, up):
    return jax.nn.silu(gate) * up


def setup_inputs(seed: int = 0, part: int = 0) -> dict:
    kx, ky, ka, kb, kg, ku, kd = jax.random.split(jax.random.key(seed), 7)
    kx, ky, ka, kb = (jax.random.fold_in(k, part) for k in (kx, ky, ka, kb))
    drawn = {
        "x": jax.random.normal(kx, (ROWS, D), jnp.float32),
        "dy": jax.random.normal(ky, (ROWS, D), jnp.float32),
        "gate": jax.random.normal(ka, (ROWS, FF), jnp.float32),
        "up": jax.random.normal(kb, (ROWS, FF), jnp.float32),
        "w_gate": jax.random.normal(kg, (D, FF), jnp.float32) * D**-0.5,
        "w_up": jax.random.normal(ku, (D, FF), jnp.float32) * D**-0.5,
        "w_down": jax.random.normal(kd, (FF, D), jnp.float32) * FF**-0.5,
    }
    return {k: v.astype(jnp.bfloat16) for k, v in drawn.items()}


def reference(x, dy, gate, up, w_gate, w_up, w_down):
    hidden, back = jax.vjp(act, gate.astype(jnp.float32), up.astype(jnp.float32))
    d_hidden = jnp.dot(dy, w_down.T, preferred_element_type=jnp.float32)
    d_gate, d_up = (g.astype(jnp.bfloat16) for g in back(d_hidden))
    dx = jnp.dot(d_gate, w_gate.T, preferred_element_type=jnp.float32) + jnp.dot(d_up, w_up.T, preferred_element_type=jnp.float32)
    dw_gate = jnp.dot(x.T, d_gate, preferred_element_type=jnp.float32)
    dw_up = jnp.dot(x.T, d_up, preferred_element_type=jnp.float32)
    dw_down = jnp.dot(hidden.astype(jnp.bfloat16).T, dy, preferred_element_type=jnp.float32)
    return tuple(g.astype(jnp.bfloat16) for g in (dx, dw_gate, dw_up, dw_down))
```

```python
import jax
import jax.numpy as jnp
from jax import lax
from jax.experimental import pallas as pl
from jax.experimental.pallas import tpu as pltpu
from jax.sharding import PartitionSpec as P

N = 2048
D = 5120
F = 1024
R = 256
CH = N // R
H, Q, E = R // 2, R // 4, R // 8
TB = 512
NB = D // TB
BF = jnp.bfloat16
F32 = jnp.float32
COMM = True
WHEN = {"p1": (1, 0), "fold": (2, 1), "mid": (4, 1), "p3": (5, 2), "fin": (6, 2), "unf": (7, 2), "ap1": (9, 2), "acore": (11, 0)}
NTYPE = ("core", "p1", "fold", "mid", "p3", "amid", "unf", "ap1", "acore")


def tb_dot(a, b):
    return lax.dot_general(a, b, (((1,), (1,)), ((), ())), preferred_element_type=F32)


def ta_dot(a, b):
    return lax.dot_general(a, b, (((0,), (0,)), ((), ())), preferred_element_type=F32)


def kernel(dy, gate, up, wg, wu, wd, x,
           dx, dwg, dwu, dwd, dgo, duo, hio,
           wdv, wgv, wuv, dyb, gb, ub, dgb, dub, hib,
           own, sb0, sb1, k1, sbf, sbm, k2, sp3, fin,
           lc, lp, lf, lm, l3,
           insem, wsem, osem, bsem, bout, finsem, ss, rs, cred):
    me = lax.axis_index("tp")
    core = lax.rem(me, 2)
    z = lax.rem(me // 2, 4)
    yy = lax.rem(me // 8, 2)
    xx = me // 16
    c0 = core == 0
    inner = jnp.logical_or(z == 1, z == 2)
    outer = jnp.logical_not(inner)
    peer = me + 1 - 2 * core
    xp = me + 16 - 32 * xx
    yp = me + 8 - 16 * yy
    bit1 = jnp.where(c0, xx, yy)
    d1 = jnp.where(c0, xp, yp)
    d3 = jnp.where(c0, yp, xp)
    dz = jnp.where(lax.rem(z, 2) == 0, me + 2, me - 2)
    dm = jnp.where(z == 1, me + 2, me - 2)
    kc = core * H
    kp = bit1 * Q
    sp = (1 - bit1) * Q
    km = jnp.where(z == 2, E, 0)
    sm = E - km
    T = {n: i for i, n in enumerate(NTYPE)}

    def rd(n, c, src, dst, dev):
        return pltpu.make_async_remote_copy(
            src_ref=src, dst_ref=dst, send_sem=ss.at[T[n], c], recv_sem=rs.at[T[n], c],
            device_id={"tp": dev}, device_id_type=pl.DeviceIdType.MESH)

    def rows(c, off, n):
        return dx.at[pl.ds(pl.multiple_of(c * R + off, 16), n)]

    def cp_core(c):
        return rd("core", c, sb0, lc.at[lax.rem(c, 2)], peer)

    def cp_p1(c):
        return rd("p1", c, sb1.at[lax.rem(c, 2)], lp.at[lax.rem(c, 3)], d1)

    def cp_fold(c):
        return rd("fold", c, sbf.at[lax.rem(c, 2)], lf.at[lax.rem(c, 3)], dz)

    def cp_mid(c):
        return rd("mid", c, sbm.at[lax.rem(c, 2)], lm.at[lax.rem(c, 2)], dm)

    def cp_p3(c):
        return rd("p3", c, sp3.at[lax.rem(c, 2)], l3.at[lax.rem(c, 2)], d3)

    def cp_amid(c):
        return rd("amid", c, fin.at[lax.rem(c, 2)], rows(c, kc + kp + km, E), dm)

    def cp_fin(c):
        s = lax.rem(c, 2)
        return pltpu.make_async_copy(fin.at[s], rows(c, kc + kp + km, E), finsem.at[s])

    def cp_unf(c):
        return rd("unf", c, rows(c, kc + kp, Q), rows(c, kc + kp, Q), dz)

    def cp_ap1(c):
        return rd("ap1", c, rows(c, kc + kp, Q), rows(c, kc + kp, Q), d1)

    def cp_acore(c):
        return rd("acore", c, rows(c, kc, H), rows(c, kc, H), peer)

    def credit(i, dev):
        pl.semaphore_signal(cred.at[i], inc=1, device_id={"tp": dev}, device_id_type=pl.DeviceIdType.MESH)

    CB = 640

    def cols(f):
        @pl.loop(0, D // CB)
        def _(j):
            f(pl.ds(pl.multiple_of(j * CB, 128), CB))

    def ds_(o, n):
        return pl.ds(pl.multiple_of(o, 16), n)

    def e_send_core(c):
        @pl.when(c >= 2)
        def _():
            pl.semaphore_wait(cred.at[0], 1)
        cp_core(c).start()

    def e_p1(c):
        cp = cp_core(c)
        cp.wait_send()
        cp.wait_recv()
        s, t, u = lax.rem(c, 2), lax.rem(c, 4), lax.rem(c, 2)

        @pl.when(c >= 2)
        def _():
            cp_p1(c - 2).wait_send()

        @pl.when(c >= 3)
        def _():
            pl.semaphore_wait(cred.at[1], 1)

        def f(cs):
            sb1[s, :, cs] = (own[ds_(sp, Q), cs] + lc[u, ds_(sp, Q), cs].astype(F32)).astype(BF)
        cols(f)
        cp_p1(c).start()

        def g(cs):
            k1[t, :, cs] = own[ds_(kp, Q), cs] + lc[u, ds_(kp, Q), cs].astype(F32)
        cols(g)

        @pl.when(c < CH - 2)
        def _():
            credit(0, peer)

    def e_fold(c):
        cp_p1(c).wait_recv()
        t, u, s = lax.rem(c, 4), lax.rem(c, 3), lax.rem(c, 2)

        @pl.when(outer)
        def _():
            @pl.when(c >= 2)
            def _():
                cp_fold(c - 2).wait_send()

            @pl.when(c >= 3)
            def _():
                pl.semaphore_wait(cred.at[2], 1)

            def f(cs):
                sbf[s, :, cs] = (k1[t, :, cs] + lp[u, :, cs].astype(F32)).astype(BF)
            cols(f)
            cp_fold(c).start()

        @pl.when(inner)
        def _():
            def f(cs):
                k1[t, :, cs] = k1[t, :, cs] + lp[u, :, cs].astype(F32)
            cols(f)

        @pl.when(c < CH - 3)
        def _():
            credit(1, d1)

    def e_mid(c):
        @pl.when(inner)
        def _():
            cp_fold(c).wait_recv()
            t, u, s = lax.rem(c, 4), lax.rem(c, 3), lax.rem(c, 2)

            @pl.when(c >= 2)
            def _():
                cp_mid(c - 2).wait_send()
                pl.semaphore_wait(cred.at[3], 1)

            def f(cs):
                sbm[s, :, cs] = (k1[t, ds_(sm, E), cs] + lf[u, ds_(sm, E), cs].astype(F32)).astype(BF)
            cols(f)
            cp_mid(c).start()

            def g(cs):
                k2[s, :, cs] = k1[t, ds_(km, E), cs] + lf[u, ds_(km, E), cs].astype(F32)
            cols(g)

            @pl.when(c < CH - 3)
            def _():
                credit(2, dz)

    def e_p3(c):
        @pl.when(inner)
        def _():
            cp_mid(c).wait_recv()
            s = lax.rem(c, 2)

            @pl.when(c >= 2)
            def _():
                cp_p3(c - 2).wait_send()
                pl.semaphore_wait(cred.at[4], 1)

            def f(cs):
                sp3[s, :, cs] = (k2[s, :, cs] + lm[s, :, cs].astype(F32)).astype(BF)
            cols(f)
            cp_p3(c).start()

            @pl.when(c < CH - 2)
            def _():
                credit(3, dm)

    def e_fin(c):
        @pl.when(inner)
        def _():
            cp_p3(c).wait_recv()
            s = lax.rem(c, 2)

            @pl.when(c >= 2)
            def _():
                cp_amid(c - 2).wait_send()

            def f(cs):
                fin[s, :, cs] = (sp3[s, :, cs].astype(F32) + l3[s, :, cs].astype(F32)).astype(BF)
            cols(f)
            cp_amid(c).start()
            cp_fin(c).start()

            @pl.when(c < CH - 2)
            def _():
                credit(4, d3)

    def e_unf(c):
        @pl.when(inner)
        def _():
            cp_fin(c).wait()
            cp_amid(c).wait_recv()
            cp_unf(c).start()
            cp_ap1(c).start()

    def e_ap1(c):
        @pl.when(outer)
        def _():
            cp_unf(c).wait_recv()
            cp_ap1(c).start()

    def e_acore(c):
        cp_ap1(c).wait_recv()
        cp_acore(c).start()

    EV = {"p1": e_p1, "fold": e_fold, "mid": e_mid, "p3": e_p3, "fin": e_fin, "unf": e_unf, "ap1": e_ap1, "acore": e_acore}

    def events(t, pos, lo, hi):
        if not COMM:
            return
        for n, (dt, ps) in WHEN.items():
            if ps != pos or hi - 1 - dt < 0 or lo - dt >= CH:
                continue
            c = t - dt

            @pl.when(jnp.logical_and(c >= 0, c < CH))
            def _(n=n, c=c):
                EV[n](c)

    if COMM:
        bar = pltpu.get_barrier_semaphore()
        for dev in (peer, d1, d3, dz):
            pl.semaphore_signal(bar, inc=1, device_id={"tp": dev}, device_id_type=pl.DeviceIdType.MESH)

        @pl.when(inner)
        def _():
            pl.semaphore_signal(bar, inc=1, device_id={"tp": dm}, device_id_type=pl.DeviceIdType.MESH)

    def ld_dy(i):
        return pltpu.make_async_copy(dy.at[pl.ds(pl.multiple_of(i * R, R), R)], dyb, insem.at[0])

    def ld_g(i):
        return pltpu.make_async_copy(gate.at[pl.ds(pl.multiple_of(i * R, R), R)], gb, insem.at[1])

    def ld_u(i):
        return pltpu.make_async_copy(up.at[pl.ds(pl.multiple_of(i * R, R), R)], ub, insem.at[2])

    def st(i, k):
        src, dst = ((dgb, dgo), (dub, duo), (hib, hio))[k]
        return pltpu.make_async_copy(src, dst.at[pl.ds(pl.multiple_of(i * R, R), R)], osem.at[k])

    lw = [pltpu.make_async_copy(wd, wdv, wsem.at[0]), pltpu.make_async_copy(wg, wgv, wsem.at[1]), pltpu.make_async_copy(wu, wuv, wsem.at[2])]
    ld_dy(0).start()
    lw[0].start()
    ld_g(0).start()
    ld_u(0).start()
    lw[1].start()
    lw[2].start()
    if COMM:
        @pl.when(inner)
        def _():
            pl.semaphore_wait(bar, 5)

        @pl.when(outer)
        def _():
            pl.semaphore_wait(bar, 4)

    def phase_a(i, _):
        @pl.when(i > 0)
        def _():
            for k in range(3):
                st(i - 1, k).wait()

        @pl.when(i == 0)
        def _():
            lw[0].wait()
        ld_dy(i).wait()
        ld_g(i).wait()
        ld_u(i).wait()

        @pl.loop(0, F // 512)
        def _(j):
            cs = pl.ds(pl.multiple_of(j * 512, 512), 512)
            dh = tb_dot(dyb[...], wdv[cs, :])
            g = gb[:, cs].astype(F32)
            u = ub[:, cs].astype(F32)
            s = 1.0 / (1.0 + jnp.exp(-g))
            gs = g * s
            dgb[:, cs] = (dh * u * (s + gs * (1.0 - s))).astype(BF)
            dub[:, cs] = (dh * gs).astype(BF)
            hib[:, cs] = (gs * u).astype(BF)

        for k in range(3):
            st(i, k).start()

        @pl.when(i < CH - 1)
        def _():
            ld_dy(i + 1).start()
            ld_g(i + 1).start()
            ld_u(i + 1).start()

        @pl.when(i == 0)
        def _():
            lw[1].wait()
            lw[2].wait()
        events(i, 0, 0, CH)

        def tblock(j):
            rs_ = pl.ds(pl.multiple_of(j * 512, 512), 512)
            t = tb_dot(dgb[...], wgv[rs_, :]) + tb_dot(dub[...], wuv[rs_, :])
            a, b = t[:H], t[H:]
            own[:, rs_] = jnp.where(c0, a, b)
            sb0[:, rs_] = jnp.where(c0, b, a).astype(BF)

        pl.loop(0, 5)(tblock)
        events(i, 1, 0, CH)
        pl.loop(5, 10)(tblock)
        if COMM:
            e_send_core(i)
        events(i, 2, 0, CH)
        return 0

    lax.fori_loop(0, CH, phase_a, 0)
    for k in range(3):
        st(CH - 1, k).wait()

    dgv, duv = wgv.at[pl.ds(0, N)], wgv.at[pl.ds(N, N)]
    hiv = wuv.at[pl.ds(0, N)]
    K2 = N // 2

    def ld_x(b):
        s = lax.rem(b, 2)
        return pltpu.make_async_copy(x.at[:, pl.ds(pl.multiple_of(b * TB, TB), TB)],
                                     wuv.at[pl.ds(N, N), pl.ds(pl.multiple_of(s * TB, TB), TB)], bsem.at[0, s])

    def ld_dyc(b, h):
        s = lax.rem(b, 2)
        return pltpu.make_async_copy(dy.at[pl.ds(h * K2, K2), pl.ds(pl.multiple_of(b * TB, TB), TB)],
                                     wdv.at[:, pl.ds(pl.multiple_of(s * 2 * TB, TB) + h * TB, TB)], bsem.at[1 + h, s])

    def out_g(b, k):
        s = lax.rem(b, 2)
        v = (wgv, wuv)[k]
        return pltpu.make_async_copy(v.at[pl.ds(pl.multiple_of(2 * N + s * TB, TB), TB)],
                                     (dwg, dwu)[k].at[pl.ds(pl.multiple_of(b * TB, TB), TB)], bout.at[k, s])

    def out_d(b):
        s = lax.rem(b, 2)
        return pltpu.make_async_copy(wdv.at[:, pl.ds(pl.multiple_of(4096 + s * TB, TB), TB)],
                                     dwd.at[:, pl.ds(pl.multiple_of(b * TB, TB), TB)], bout.at[2, s])

    lb = [pltpu.make_async_copy(dgo, dgv, wsem.at[0]), pltpu.make_async_copy(duo, duv, wsem.at[1]), pltpu.make_async_copy(hio, hiv, wsem.at[2])]
    lb[0].start()
    ld_x(0).start()
    lb[1].start()
    lb[2].start()
    ld_dyc(0, 0).start()
    ld_dyc(0, 1).start()

    def phase_b(b, _):
        t = b + CH
        s = lax.rem(b, 2)

        @pl.when(b < NB - 1)
        def _():
            ld_x(b + 1).start()
            ld_dyc(b + 1, 0).start()
            ld_dyc(b + 1, 1).start()

        @pl.when(b == 0)
        def _():
            lb[0].wait()
        ld_x(b).wait()
        xs = pl.ds(pl.multiple_of(s * TB, TB), TB)
        for k in range(2):
            @pl.when(b >= 2)
            def _():
                out_g(b - 2, k).wait()

            if k == 1:
                @pl.when(b == 0)
                def _():
                    lb[1].wait()
            r = ta_dot(wuv[pl.ds(N, N), xs], (dgv, duv)[k][...])
            (wgv, wuv)[k][pl.ds(pl.multiple_of(2 * N + s * TB, TB), TB), :] = r.astype(BF)
            out_g(b, k).start()
            events(t, k, CH, CH + NB)

        @pl.when(b >= 2)
        def _():
            out_d(b - 2).wait()

        @pl.when(b == 0)
        def _():
            lb[2].wait()
        ld_dyc(b, 0).wait()
        ld_dyc(b, 1).wait()
        y0 = wdv[:, pl.ds(pl.multiple_of(s * 2 * TB, TB), TB)]
        y1 = wdv[:, pl.ds(pl.multiple_of(s * 2 * TB, TB) + TB, TB)]
        r = ta_dot(hiv[pl.ds(0, K2), :], y0) + ta_dot(hiv[pl.ds(K2, K2), :], y1)
        wdv[:, pl.ds(pl.multiple_of(4096 + s * TB, TB), TB)] = r.astype(BF)
        out_d(b).start()
        events(t, 2, CH, CH + NB)
        return 0

    lax.fori_loop(0, NB, phase_b, 0)
    last = CH + max(dt for dt, _ in WHEN.values())
    if COMM and last > CH + NB:
        def drain(t, _):
            for p in range(3):
                events(t, p, CH + NB, last)
            return 0
        lax.fori_loop(CH + NB, last, drain, 0)

    for b in (NB - 2, NB - 1):
        out_g(b, 0).wait()
        out_g(b, 1).wait()
        out_d(b).wait()
    if COMM:
        def tail(c, _):
            cp_acore(c).wait_recv()
            cp_acore(c).wait_send()
            cp_ap1(c).wait_send()

            @pl.when(inner)
            def _():
                cp_unf(c).wait_send()
            return 0
        lax.fori_loop(0, CH, tail, 0)
        for c in (CH - 2, CH - 1):
            cp_p1(c).wait_send()

            @pl.when(inner)
            def _():
                cp_mid(c).wait_send()
                cp_p3(c).wait_send()
                cp_amid(c).wait_send()

            @pl.when(outer)
            def _():
                cp_fold(c).wait_send()


def call(dy, gate, up, wg, wu, wd, x):
    s = jax.ShapeDtypeStruct
    V = pltpu.VMEM
    S = pltpu.SemaphoreType
    any_ = pl.BlockSpec(memory_space=pl.ANY)
    return pl.pallas_call(
        kernel,
        in_specs=[any_] * 7,
        out_specs=[any_] * 7,
        out_shape=[s((N, D), BF), s((D, F), BF), s((D, F), BF), s((F, D), BF), s((N, F), BF), s((N, F), BF), s((N, F), BF)],
        scratch_shapes=[
            V((F, D), BF), V((D, F), BF), V((D, F), BF), V((R, D), BF), V((R, F), BF), V((R, F), BF),
            V((R, F), BF), V((R, F), BF), V((R, F), BF),
            V((H, D), F32), V((H, D), BF), V((2, Q, D), BF), V((4, Q, D), F32), V((2, Q, D), BF), V((2, E, D), BF),
            V((2, E, D), F32), V((2, E, D), BF), V((2, E, D), BF),
            V((2, H, D), BF), V((3, Q, D), BF), V((3, Q, D), BF), V((2, E, D), BF), V((2, E, D), BF),
            S.DMA((3,)), S.DMA((3,)), S.DMA((3,)), S.DMA((3, 2)), S.DMA((3, 2)), S.DMA((2,)),
            S.DMA((len(NTYPE), CH)), S.DMA((len(NTYPE), CH)), S.REGULAR((5,)),
        ],
        compiler_params=pltpu.CompilerParams(collective_id=0, has_side_effects=True, vmem_limit_bytes=67043328) if COMM
        else pltpu.CompilerParams(vmem_limit_bytes=67043328),
        cost_estimate=pl.CostEstimate(flops=6 * 2 * N * D * F, bytes_accessed=200 * 2**20, transcendentals=N * F),
        name="mlp_bwd",
    )(dy, gate, up, wg, wu, wd, x)


def solution(mesh):
    def step(x, dy, gate, up, w_gate, w_up, w_down):
        dx, dwg, dwu, dwd, *_ = call(dy, gate, up, w_gate, w_up, w_down, x)
        return dx, dwg, dwu, dwd

    tokens, columns, rows = P("dp", None), P(None, "tp"), P("tp", None)
    return jax.shard_map(
        step,
        mesh=mesh,
        in_specs=(tokens, tokens, P("dp", "tp"), P("dp", "tp"), columns, columns, rows),
        out_specs=(tokens, P("dp", "tp"), P("dp", "tp"), P(("dp", "tp"), None)),
        check_vma=False,
    )
```

```python
import jax
import jax.numpy as jnp
from jax import lax
from jax.experimental import pallas as pl
from jax.experimental.pallas import tpu as pltpu
from jax.sharding import PartitionSpec as P

N = 2048
D = 5120
F = 1024
R = 256
NT = N // R
RC = 128
CH = N // RC
H, Q, E = RC // 2, RC // 4, RC // 8
TB = 512
NB = D // TB
PT = 6
DEP = 4
KD = 12
CB = 5120
FAKE = False
DOWN2 = False
FS = ()
NOEW = False
BF = jnp.bfloat16
F32 = jnp.float32
COMM = True
COMP = True
OFF = dict(p1=(7, 7), s1=(10, 12), s2=(13, 15), s3=(17, 18), s4=(23, 24), s5=(26, 31), a1=(30, 35), a2=(36, 39), a3=(45, 49), a4=(56, 56))
NTYPE = ("core", "p1", "s1", "s2", "s3", "p3", "a1", "a2", "a3", "ap1", "acore")


def tb_dot(a, b):
    return lax.dot_general(a, b, (((1,), (1,)), ((), ())), preferred_element_type=F32)


def ta_dot(a, b):
    return lax.dot_general(a, b, (((0,), (0,)), ((), ())), preferred_element_type=F32)


def kernel(dy, gate, up, wg, wu, wd, x,
           dx, dwg, dwu, dwd, dgo, duo, hio,
           wdv, wgv, wuv, dyb, gb, ub, dgb, dub, hib,
           own, sb0, sb1, k1, b1, b2, b3, b4, fin,
           lc, lp, l1, l2, l3, l4,
           insem, wsem, osem, bsem, bout, finsem, ss, rs, cred):
    me = lax.axis_index("tp")
    core = lax.rem(me, 2)
    z = lax.rem(me // 2, 4)
    yy = lax.rem(me // 8, 2)
    xx = me // 16
    c0 = core == 0
    inner = jnp.logical_or(z == 1, z == 2)
    outer = jnp.logical_not(inner)
    peer = me + 1 - 2 * core
    xp = me + 16 - 32 * xx
    yp = me + 8 - 16 * yy
    bit1 = jnp.where(c0, xx, yy)
    d1 = jnp.where(c0, xp, yp)
    d3 = jnp.where(c0, yp, xp)
    dz = jnp.where(lax.rem(z, 2) == 0, me + 2, me - 2)
    dm = jnp.where(z == 1, me + 2, me - 2)
    kc = core * H
    kp = bit1 * Q
    sp = (1 - bit1) * Q
    nr = jnp.where(z <= 1, 0, E)
    fr = E - nr
    T = {n: i for i, n in enumerate(NTYPE)}

    class Dummy:
        def start(self): pass
        wait_send = wait_recv = wait = start

    def rd(n, c, src, dst, dev):
        if FAKE or n in FS:
            return Dummy()
        return pltpu.make_async_remote_copy(
            src_ref=src, dst_ref=dst, send_sem=ss.at[T[n], c], recv_sem=rs.at[T[n], c],
            device_id={"tp": dev}, device_id_type=pl.DeviceIdType.MESH)

    def rows(c, off, n):
        return dx.at[pl.ds(pl.multiple_of(c * RC + off, 16), n)]

    def m(c, k=DEP):
        return lax.rem(c, k)

    def cp(n, c):
        s = m(c)
        near, far, both = (rows(c, kc + kp + nr, E), rows(c, kc + kp + fr, E), rows(c, kc + kp, Q))
        if n == "core":
            return rd(n, c, sb0.at[m(c, 2)], lc.at[s], peer)
        if n == "p1":
            return rd(n, c, sb1.at[s], lp.at[s], d1)
        if n == "s1":
            return rd(n, c, b1.at[s], l1.at[s], dz)
        if n == "s2":
            return rd(n, c, b2.at[s], l2.at[s], dm)
        if n == "s3":
            return rd(n, c, b3.at[s], l3.at[s], dz)
        if n == "p3":
            return rd(n, c, b4.at[s], l4.at[s], d3)
        if n == "a1":
            return rd(n, c, fin.at[s], near, dz)
        if n == "a2":
            return rd(n, c, near, near, dm)
        if n == "a3":
            return rd(n, c, far, far, dz)
        if n == "ap1":
            return rd(n, c, both, both, d1)
        return rd(n, c, rows(c, kc, H), rows(c, kc, H), peer)

    def cp_fin(c):
        s = m(c)
        return pltpu.make_async_copy(fin.at[s], rows(c, kc + kp + nr, E), finsem.at[s])

    def recv_a(n, c):
        near, far = rows(c, kc + kp + nr, E), rows(c, kc + kp + fr, E)
        r = {"a1": near, "a2": far, "a3": far}[n]
        rd(n, c, r, r, peer).wait_recv()

    CI = {"core": 0, "p1": 1, "s1": 2, "s2": 3, "s3": 4, "p3": 5}

    def take(n, c):
        if FAKE or n in FS:
            return
        @pl.when(c >= DEP)
        def _():
            pl.semaphore_wait(cred.at[CI[n]], 1)

    def give(n, c, dev):
        if FAKE or n in FS:
            return
        @pl.when(c < CH - DEP)
        def _():
            pl.semaphore_signal(cred.at[CI[n]], inc=1, device_id={"tp": dev}, device_id_type=pl.DeviceIdType.MESH)

    def free(n, c):
        @pl.when(c >= DEP)
        def _():
            cp(n, c - DEP).wait_send()


    def cols(f):
        if NOEW:
            return
        @pl.loop(0, D // CB)
        def _(j):
            f(pl.ds(pl.multiple_of(j * CB, 128), CB))

    def ds_(o, n):
        return pl.ds(pl.multiple_of(o, 16), n)

    def f32(v):
        return v.astype(F32)

    def e_send_core(c):
        take("core", c)
        cp("core", c).start()

    def e_p1(c):
        cp("core", c).wait_send()
        cp("core", c).wait_recv()
        s, t, o = m(c), m(c, KD), m(c, 2)
        free("p1", c)
        take("p1", c)

        def f(cs):
            sb1[s, :, cs] = (own[o, ds_(sp, Q), cs] + f32(lc[s, ds_(sp, Q), cs])).astype(BF)
        cols(f)
        cp("p1", c).start()

        def g(cs):
            k1[t, :, cs] = own[o, ds_(kp, Q), cs] + f32(lc[s, ds_(kp, Q), cs])
        cols(g)
        give("core", c, peer)

    def e_s1(c):
        cp("p1", c).wait_recv()
        s, t = m(c), m(c, KD)

        @pl.when(outer)
        def _():
            free("s1", c)
            take("s1", c)

            def f(cs):
                b1[s, :, cs] = (k1[t, ds_(fr, E), cs] + f32(lp[s, ds_(fr, E), cs])).astype(BF)
            cols(f)
            cp("s1", c).start()

            def g(cs):
                k1[t, ds_(nr, E), cs] = k1[t, ds_(nr, E), cs] + f32(lp[s, ds_(nr, E), cs])
            cols(g)

        @pl.when(inner)
        def _():
            def f(cs):
                k1[t, :, cs] = k1[t, :, cs] + f32(lp[s, :, cs])
            cols(f)

        give("p1", c, d1)

    def hop(n_in, n_out, c, role, half, land, buf, giver):
        @pl.when(role)
        def _():
            cp(n_in, c).wait_recv()
            s, t = m(c), m(c, KD)
            free(n_out, c)
            take(n_out, c)

            def f(cs):
                buf[s, :, cs] = (k1[t, ds_(half, E), cs] + f32(land[s, :, cs])).astype(BF)
            cols(f)
            cp(n_out, c).start()
            give(n_in, c, giver)

    def e_s2(c):
        hop("s1", "s2", c, inner, fr, l1, b2, dz)

    def e_s3(c):
        hop("s2", "s3", c, inner, nr, l2, b3, dm)

    def e_s4(c):
        hop("s3", "p3", c, outer, nr, l3, b4, dz)

    def e_s5(c):
        @pl.when(outer)
        def _():
            cp("p3", c).wait_recv()
            s = m(c)
            free("a1", c)

            def f(cs):
                fin[s, :, cs] = (f32(b4[s, :, cs]) + f32(l4[s, :, cs])).astype(BF)
            cols(f)
            cp("a1", c).start()
            cp_fin(c).start()
            give("p3", c, d3)

    def e_a1(c):
        @pl.when(inner)
        def _():
            recv_a("a1", c)
            cp("a2", c).start()

        @pl.when(outer)
        def _():
            cp_fin(c).wait()

    def e_a2(c):
        @pl.when(inner)
        def _():
            recv_a("a2", c)
            cp("a3", c).start()
            cp("ap1", c).start()

    def e_a3(c):
        @pl.when(outer)
        def _():
            recv_a("a3", c)
            cp("ap1", c).start()

    def e_a4(c):
        cp("ap1", c).wait_recv()
        cp("acore", c).start()

    EV = dict(p1=e_p1, s1=e_s1, s2=e_s2, s3=e_s3, s4=e_s4, s5=e_s5, a1=e_a1, a2=e_a2, a3=e_a3, a4=e_a4)

    def events(t, pos, lo, hi):
        if not COMM:
            return
        for n, offs in OFF.items():
            for odd, off in enumerate(offs):
                dt, ps = divmod(off, PT)
                if ps != pos or hi - 1 - dt < 0 or lo - dt >= NT:
                    continue
                i = t - dt

                @pl.when(jnp.logical_and(i >= 0, i < NT))
                def _(n=n, i=i, odd=odd):
                    EV[n](2 * i + odd)

    if COMM:
        bar = pltpu.get_barrier_semaphore()
        for dev in (peer, d1, dz, jnp.where(inner, dm, d3)):
            pl.semaphore_signal(bar, inc=1, device_id={"tp": dev}, device_id_type=pl.DeviceIdType.MESH)

    def ld_dy(i):
        return pltpu.make_async_copy(dy.at[pl.ds(pl.multiple_of(i * R, R), R)], dyb, insem.at[0])

    def ld_g(i):
        return pltpu.make_async_copy(gate.at[pl.ds(pl.multiple_of(i * R, R), R)], gb, insem.at[1])

    def ld_u(i):
        return pltpu.make_async_copy(up.at[pl.ds(pl.multiple_of(i * R, R), R)], ub, insem.at[2])

    def st(i, k):
        src, dst = ((dgb, dgo), (dub, duo), (hib, hio))[k]
        return pltpu.make_async_copy(src, dst.at[pl.ds(pl.multiple_of(i * R, R), R)], osem.at[k])

    lw = [pltpu.make_async_copy(wd, wdv, wsem.at[0]), pltpu.make_async_copy(wg, wgv, wsem.at[1]), pltpu.make_async_copy(wu, wuv, wsem.at[2])]
    ld_dy(0).start()
    lw[0].start()
    ld_g(0).start()
    ld_u(0).start()
    lw[1].start()
    lw[2].start()
    if COMM:
        pl.semaphore_wait(bar, 4)

    def phase_a(i, _):
        @pl.when(i > 0)
        def _():
            for k in range(3):
                st(i - 1, k).wait()

        @pl.when(i == 0)
        def _():
            lw[0].wait()
        ld_dy(i).wait()
        ld_g(i).wait()
        ld_u(i).wait()

        def dblock(j):
            cs = pl.ds(j * 512, 512)
            dh = tb_dot(dyb[...], wdv[cs, :]) if COMP else dyb[:, 0:512].astype(F32)
            g = gb[:, cs].astype(F32)
            u = ub[:, cs].astype(F32)
            s = 1.0 / (1.0 + jnp.exp(-g))
            gs = g * s
            dgb[:, cs] = (dh * u * (s + gs * (1.0 - s))).astype(BF)
            dub[:, cs] = (dh * gs).astype(BF)
            hib[:, cs] = (gs * u).astype(BF)

        dblock(0)
        events(i, 0, 0, NT)
        dblock(1)
        for k in range(3):
            st(i, k).start()

        @pl.when(i < NT - 1)
        def _():
            ld_dy(i + 1).start()
            ld_g(i + 1).start()
            ld_u(i + 1).start()

        events(i, 1, 0, NT)

        @pl.when(i == 0)
        def _():
            lw[1].wait()
            lw[2].wait()

        def tblock(j):
            rs_ = pl.ds(pl.multiple_of(j * 512, 512), 512)
            t = tb_dot(dgb[...], wgv[rs_, :]) + tb_dot(dub[...], wuv[rs_, :]) if COMP else dyb[:, rs_].astype(F32)
            for o in range(2):
                a, b = t[2 * o * H:(2 * o + 1) * H], t[(2 * o + 1) * H:(2 * o + 2) * H]
                own[o, :, rs_] = jnp.where(c0, a, b)
                sb0[o, :, rs_] = jnp.where(c0, b, a).astype(BF)

        for p, (lo, hi) in enumerate(((0, 3), (3, 5), (5, 8), (8, 10))):
            pl.loop(lo, hi)(tblock)
            if p == 3 and COMM:
                e_send_core(2 * i)
                e_send_core(2 * i + 1)
            events(i, 2 + p, 0, NT)
        return 0

    lax.fori_loop(0, NT, phase_a, 0)
    for k in range(3):
        st(NT - 1, k).wait()

    dgv, duv = wgv.at[pl.ds(0, N)], wgv.at[pl.ds(N, N)]
    hiv = wuv.at[pl.ds(0, N)]
    K2 = N // 2

    def ld_x(b):
        s = lax.rem(b, 2)
        return pltpu.make_async_copy(x.at[:, pl.ds(pl.multiple_of(b * TB, TB), TB)],
                                     wuv.at[pl.ds(N, N), pl.ds(pl.multiple_of(s * TB, TB), TB)], bsem.at[0, s])

    def ld_dyc(b, h):
        s = lax.rem(b, 2)
        return pltpu.make_async_copy(dy.at[pl.ds(h * K2, K2), pl.ds(pl.multiple_of(b * TB, TB), TB)],
                                     wdv.at[:, pl.ds(pl.multiple_of(s * 2 * TB, TB) + h * TB, TB)], bsem.at[1 + h, s])

    def out_g(b, k):
        s = lax.rem(b, 2)
        v = (wgv, wuv)[k]
        return pltpu.make_async_copy(v.at[pl.ds(pl.multiple_of(2 * N + s * TB, TB), TB)],
                                     (dwg, dwu)[k].at[pl.ds(pl.multiple_of(b * TB, TB), TB)], bout.at[k, s])

    def out_d(b):
        s = lax.rem(b, 2)
        return pltpu.make_async_copy(wdv.at[:, pl.ds(pl.multiple_of(4096 + s * TB, TB), TB)],
                                     dwd.at[:, pl.ds(pl.multiple_of(b * TB, TB), TB)], bout.at[2, s])

    lb = [pltpu.make_async_copy(dgo, dgv, wsem.at[0]), pltpu.make_async_copy(duo, duv, wsem.at[1]), pltpu.make_async_copy(hio, hiv, wsem.at[2])]
    lb[0].start()
    ld_x(0).start()
    lb[1].start()
    if not DOWN2:
        lb[2].start()
        ld_dyc(0, 0).start()
        ld_dyc(0, 1).start()

    def phase_b(b, _):
        t = b + NT
        s = lax.rem(b, 2)

        @pl.when(b < NB - 1)
        def _():
            ld_x(b + 1).start()
            if not DOWN2:
                ld_dyc(b + 1, 0).start()
                ld_dyc(b + 1, 1).start()

        @pl.when(b == 0)
        def _():
            lb[0].wait()
        ld_x(b).wait()
        xs = pl.ds(pl.multiple_of(s * TB, TB), TB)
        for k in range(2):
            @pl.when(b >= 2)
            def _():
                out_g(b - 2, k).wait()

            if k == 1:
                @pl.when(b == 0)
                def _():
                    lb[1].wait()
            r = ta_dot(wuv[pl.ds(N, N), xs], (dgv, duv)[k][...]) if COMP else wuv[0:512, :].astype(F32)
            (wgv, wuv)[k][pl.ds(pl.multiple_of(2 * N + s * TB, TB), TB), :] = r.astype(BF)
            out_g(b, k).start()
            events(t, 2 * k, NT, NT + NB)
            events(t, 2 * k + 1, NT, NT + NB)

        if not DOWN2:
            @pl.when(b >= 2)
            def _():
                out_d(b - 2).wait()

            @pl.when(b == 0)
            def _():
                lb[2].wait()
            ld_dyc(b, 0).wait()
            ld_dyc(b, 1).wait()
            y0 = wdv[:, pl.ds(pl.multiple_of(s * 2 * TB, TB), TB)]
            y1 = wdv[:, pl.ds(pl.multiple_of(s * 2 * TB, TB) + TB, TB)]
            r = ta_dot(hiv[pl.ds(0, K2), :], y0) + ta_dot(hiv[pl.ds(K2, K2), :], y1) if COMP else y0.astype(F32)
            wdv[:, pl.ds(pl.multiple_of(4096 + s * TB, TB), TB)] = r.astype(BF)
            out_d(b).start()
        events(t, 4, NT, NT + NB)
        events(t, 5, NT, NT + NB)
        return 0

    lax.fori_loop(0, NB, phase_b, 0)
    last = NT + max(o for v in OFF.values() for o in v) // PT
    if COMM and last > NT + NB:
        def drain(t, _):
            for p in range(PT):
                events(t, p, NT + NB, last)
            return 0
        lax.fori_loop(NT + NB, last, drain, 0)

    for b in (NB - 2, NB - 1):
        out_g(b, 0).wait()
        out_g(b, 1).wait()
        if not DOWN2:
            out_d(b).wait()
    if COMM:
        def tail(c, _):
            cp("acore", c).wait_recv()
            cp("acore", c).wait_send()
            cp("ap1", c).wait_send()

            @pl.when(inner)
            def _():
                cp("a2", c).wait_send()
                cp("a3", c).wait_send()
            return 0
        lax.fori_loop(0, CH, tail, 0)

        def tail2(c, _):
            cp("p1", c).wait_send()

            @pl.when(inner)
            def _():
                cp("s2", c).wait_send()
                cp("s3", c).wait_send()

            @pl.when(outer)
            def _():
                cp("s1", c).wait_send()
                cp("p3", c).wait_send()
                cp("a1", c).wait_send()
            return 0
        lax.fori_loop(CH - DEP, CH, tail2, 0)


def call(dy, gate, up, wg, wu, wd, x):
    s = jax.ShapeDtypeStruct
    V = pltpu.VMEM
    S = pltpu.SemaphoreType
    any_ = pl.BlockSpec(memory_space=pl.ANY)
    return pl.pallas_call(
        kernel,
        in_specs=[any_] * 7,
        out_specs=[any_] * 7,
        out_shape=[s((N, D), BF), s((D, F), BF), s((D, F), BF), s((F, D), BF), s((N, F), BF), s((N, F), BF), s((N, F), BF)],
        scratch_shapes=[
            V((F, D), BF), V((D, F), BF), V((D, F), BF), V((R, D), BF), V((R, F), BF), V((R, F), BF),
            V((R, F), BF), V((R, F), BF), V((R, F), BF),
            V((2, H, D), F32), V((2, H, D), BF), V((DEP, Q, D), BF), V((KD, Q, D), F32),
            V((DEP, E, D), BF), V((DEP, E, D), BF), V((DEP, E, D), BF), V((DEP, E, D), BF), V((DEP, E, D), BF),
            V((DEP, H, D), BF), V((DEP, Q, D), BF), V((DEP, E, D), BF), V((DEP, E, D), BF), V((DEP, E, D), BF), V((DEP, E, D), BF),
            S.DMA((3,)), S.DMA((3,)), S.DMA((3,)), S.DMA((3, 2)), S.DMA((3, 2)), S.DMA((DEP,)),
            S.DMA((len(NTYPE), CH)), S.DMA((len(NTYPE), CH)), S.REGULAR((6,)),
        ],
        compiler_params=pltpu.CompilerParams(collective_id=0, has_side_effects=True, vmem_limit_bytes=67043328) if COMM
        else pltpu.CompilerParams(vmem_limit_bytes=67043328),
        cost_estimate=pl.CostEstimate(flops=6 * 2 * N * D * F, bytes_accessed=200 * 2**20, transcendentals=N * F),
        name="mlp_bwd",
    )(dy, gate, up, wg, wu, wd, x)


def finish_kernel(hi, dy, dx, dwg, dwu, dwd, odx, odwg, odwu, odwd):
    odx[...] = dx[...]
    odwg[...] = dwg[...]
    odwu[...] = dwu[...]
    if DOWN2:
        odwd[...] = ta_dot(hi[...], dy[...]).astype(BF)
    else:
        odwd[...] = dwd[...]


def finish(hi, dy, dx, dwg, dwu, dwd):
    s = jax.ShapeDtypeStruct
    col = lambda n: pl.BlockSpec((n, TB), lambda j: (0, j))
    row = pl.BlockSpec((TB, F), lambda j: (j, 0))
    any_ = pl.BlockSpec(memory_space=pl.ANY)
    return pl.pallas_call(
        finish_kernel,
        grid=(NB,),
        in_specs=[pl.BlockSpec((N, F), lambda j: (0, 0)) if DOWN2 else any_, col(N) if DOWN2 else any_, col(N), row, row, any_ if DOWN2 else col(F)],
        out_specs=[col(N), row, row, col(F)],
        out_shape=[s((N, D), BF), s((D, F), BF), s((D, F), BF), s((F, D), BF)],
        compiler_params=pltpu.CompilerParams(vmem_limit_bytes=60 * 2**20),
        cost_estimate=pl.CostEstimate(flops=2 * N * D * F, bytes_accessed=118 * 2**20, transcendentals=0),
        name="finish",
    )(hi, dy, dx, dwg, dwu, dwd)


def solution(mesh):
    def step(x, dy, gate, up, w_gate, w_up, w_down):
        dx, dwg, dwu, dwd, _, _, hi = call(dy, gate, up, w_gate, w_up, w_down, x)
        return finish(hi, dy, dx, dwg, dwu, dwd)

    tokens, columns, rows = P("dp", None), P(None, "tp"), P("tp", None)
    return jax.shard_map(
        step,
        mesh=mesh,
        in_specs=(tokens, tokens, P("dp", "tp"), P("dp", "tp"), columns, columns, rows),
        out_specs=(tokens, P("dp", "tp"), P("dp", "tp"), P(("dp", "tp"), None)),
        check_vma=False,
    )
```

```python
import jax
import jax.numpy as jnp
from jax import lax
from jax.experimental import pallas as pl
from jax.experimental.pallas import tpu as pltpu
from jax.sharding import PartitionSpec as P

N = 2048
D = 5120
F = 1024
R = 256
NT = N // R
RC = 128
CH = N // RC
H, Q, E = RC // 2, RC // 4, RC // 8
TB = 512
NB = D // TB
PT = 6
DEP = 4
KD = 12
CB = 5120
FAKE = False
DOWN2 = False
FS = ()
NOEW = False
BF = jnp.bfloat16
F32 = jnp.float32
COMM = True
COMP = True
OFF = dict(p1=(7, 7), s1=(10, 12), s2=(13, 15), s3=(17, 18), s4=(23, 24), s5=(26, 31), a1=(30, 35), a2=(36, 39), a3=(45, 49), a4=(56, 56))
NTYPE = ("core", "p1", "s1", "s2", "s3", "p3", "a1", "a2", "a3", "ap1", "acore")


def tb_dot(a, b):
    return lax.dot_general(a, b, (((1,), (1,)), ((), ())), preferred_element_type=F32)


def ta_dot(a, b):
    return lax.dot_general(a, b, (((0,), (0,)), ((), ())), preferred_element_type=F32)


def kernel(dy, gate, up, wg, wu, wd, x,
           dx, dwg, dwu, dwd, dgo, duo, hio,
           wdv, wgv, wuv, dyb, gb, ub, dgb, dub, hib,
           own, sb0, sb1, k1, b1, b2, b3, b4, fin,
           lc, lp, l1, l2, l3, l4,
           insem, wsem, osem, bsem, bout, finsem, ss, rs, cred):
    me = lax.axis_index("tp")
    core = lax.rem(me, 2)
    z = lax.rem(me // 2, 4)
    yy = lax.rem(me // 8, 2)
    xx = me // 16
    c0 = core == 0
    inner = jnp.logical_or(z == 1, z == 2)
    outer = jnp.logical_not(inner)
    peer = me + 1 - 2 * core
    xp = me + 16 - 32 * xx
    yp = me + 8 - 16 * yy
    bit1 = jnp.where(c0, xx, yy)
    d1 = jnp.where(c0, xp, yp)
    d3 = jnp.where(c0, yp, xp)
    dz = jnp.where(lax.rem(z, 2) == 0, me + 2, me - 2)
    dm = jnp.where(z == 1, me + 2, me - 2)
    kc = core * H
    kp = bit1 * Q
    sp = (1 - bit1) * Q
    nr = jnp.where(z <= 1, 0, E)
    fr = E - nr
    T = {n: i for i, n in enumerate(NTYPE)}

    class Dummy:
        def start(self): pass
        wait_send = wait_recv = wait = start

    def rd(n, c, src, dst, dev):
        if FAKE or n in FS:
            return Dummy()
        return pltpu.make_async_remote_copy(
            src_ref=src, dst_ref=dst, send_sem=ss.at[T[n], c], recv_sem=rs.at[T[n], c],
            device_id={"tp": dev}, device_id_type=pl.DeviceIdType.MESH)

    def rows(c, off, n):
        return dx.at[pl.ds(pl.multiple_of(c * RC + off, 16), n)]

    def m(c, k=DEP):
        return lax.rem(c, k)

    def cp(n, c):
        s = m(c)
        near, far, both = (rows(c, kc + kp + nr, E), rows(c, kc + kp + fr, E), rows(c, kc + kp, Q))
        if n == "core":
            return rd(n, c, sb0.at[m(c, 2)], lc.at[s], peer)
        if n == "p1":
            return rd(n, c, sb1.at[s], lp.at[s], d1)
        if n == "s1":
            return rd(n, c, b1.at[s], l1.at[s], dz)
        if n == "s2":
            return rd(n, c, b2.at[s], l2.at[s], dm)
        if n == "s3":
            return rd(n, c, b3.at[s], l3.at[s], dz)
        if n == "p3":
            return rd(n, c, b4.at[s], l4.at[s], d3)
        if n == "a1":
            return rd(n, c, fin.at[s], near, dz)
        if n == "a2":
            return rd(n, c, near, near, dm)
        if n == "a3":
            return rd(n, c, far, far, dz)
        if n == "ap1":
            return rd(n, c, both, both, d1)
        return rd(n, c, rows(c, kc, H), rows(c, kc, H), peer)

    def cp_fin(c):
        s = m(c)
        return pltpu.make_async_copy(fin.at[s], rows(c, kc + kp + nr, E), finsem.at[s])

    def recv_a(n, c):
        near, far = rows(c, kc + kp + nr, E), rows(c, kc + kp + fr, E)
        r = {"a1": near, "a2": far, "a3": far}[n]
        rd(n, c, r, r, peer).wait_recv()

    CI = {"core": 0, "p1": 1, "s1": 2, "s2": 3, "s3": 4, "p3": 5}

    def take(n, c):
        if FAKE or n in FS:
            return
        @pl.when(c >= DEP)
        def _():
            pl.semaphore_wait(cred.at[CI[n]], 1)

    def give(n, c, dev):
        if FAKE or n in FS:
            return
        @pl.when(c < CH - DEP)
        def _():
            pl.semaphore_signal(cred.at[CI[n]], inc=1, device_id={"tp": dev}, device_id_type=pl.DeviceIdType.MESH)

    def free(n, c):
        @pl.when(c >= DEP)
        def _():
            cp(n, c - DEP).wait_send()


    def cols(f):
        if NOEW:
            return
        @pl.loop(0, D // CB)
        def _(j):
            f(pl.ds(pl.multiple_of(j * CB, 128), CB))

    def ds_(o, n):
        return pl.ds(pl.multiple_of(o, 16), n)

    def f32(v):
        return v.astype(F32)

    def e_send_core(c):
        take("core", c)
        cp("core", c).start()

    def e_p1(c):
        cp("core", c).wait_send()
        cp("core", c).wait_recv()
        s, t, o = m(c), m(c, KD), m(c, 2)
        free("p1", c)
        take("p1", c)

        def f(cs):
            sb1[s, :, cs] = (own[o, ds_(sp, Q), cs] + f32(lc[s, ds_(sp, Q), cs])).astype(BF)
        cols(f)
        cp("p1", c).start()

        def g(cs):
            k1[t, :, cs] = own[o, ds_(kp, Q), cs] + f32(lc[s, ds_(kp, Q), cs])
        cols(g)
        give("core", c, peer)

    def e_s1(c):
        cp("p1", c).wait_recv()
        s, t = m(c), m(c, KD)

        @pl.when(outer)
        def _():
            free("s1", c)
            take("s1", c)

            def f(cs):
                b1[s, :, cs] = (k1[t, ds_(fr, E), cs] + f32(lp[s, ds_(fr, E), cs])).astype(BF)
            cols(f)
            cp("s1", c).start()

            def g(cs):
                k1[t, ds_(nr, E), cs] = k1[t, ds_(nr, E), cs] + f32(lp[s, ds_(nr, E), cs])
            cols(g)

        @pl.when(inner)
        def _():
            def f(cs):
                k1[t, :, cs] = k1[t, :, cs] + f32(lp[s, :, cs])
            cols(f)

        give("p1", c, d1)

    def hop(n_in, n_out, c, role, half, land, buf, giver):
        @pl.when(role)
        def _():
            cp(n_in, c).wait_recv()
            s, t = m(c), m(c, KD)
            free(n_out, c)
            take(n_out, c)

            def f(cs):
                buf[s, :, cs] = (k1[t, ds_(half, E), cs] + f32(land[s, :, cs])).astype(BF)
            cols(f)
            cp(n_out, c).start()
            give(n_in, c, giver)

    def e_s2(c):
        hop("s1", "s2", c, inner, fr, l1, b2, dz)

    def e_s3(c):
        hop("s2", "s3", c, inner, nr, l2, b3, dm)

    def e_s4(c):
        hop("s3", "p3", c, outer, nr, l3, b4, dz)

    def e_s5(c):
        @pl.when(outer)
        def _():
            cp("p3", c).wait_recv()
            s = m(c)
            free("a1", c)

            def f(cs):
                fin[s, :, cs] = (f32(b4[s, :, cs]) + f32(l4[s, :, cs])).astype(BF)
            cols(f)
            cp("a1", c).start()
            cp_fin(c).start()
            give("p3", c, d3)

    def e_a1(c):
        @pl.when(inner)
        def _():
            recv_a("a1", c)
            cp("a2", c).start()

        @pl.when(outer)
        def _():
            cp_fin(c).wait()

    def e_a2(c):
        @pl.when(inner)
        def _():
            recv_a("a2", c)
            cp("a3", c).start()
            cp("ap1", c).start()

    def e_a3(c):
        @pl.when(outer)
        def _():
            recv_a("a3", c)
            cp("ap1", c).start()

    def e_a4(c):
        cp("ap1", c).wait_recv()
        cp("acore", c).start()

    EV = dict(p1=e_p1, s1=e_s1, s2=e_s2, s3=e_s3, s4=e_s4, s5=e_s5, a1=e_a1, a2=e_a2, a3=e_a3, a4=e_a4)

    def events(t, pos, lo, hi):
        if not COMM:
            return
        for n, offs in OFF.items():
            for odd, off in enumerate(offs):
                dt, ps = divmod(off, PT)
                if ps != pos or hi - 1 - dt < 0 or lo - dt >= NT:
                    continue
                i = t - dt

                @pl.when(jnp.logical_and(i >= 0, i < NT))
                def _(n=n, i=i, odd=odd):
                    EV[n](2 * i + odd)

    if COMM:
        bar = pltpu.get_barrier_semaphore()
        for dev in (peer, d1, dz, jnp.where(inner, dm, d3)):
            pl.semaphore_signal(bar, inc=1, device_id={"tp": dev}, device_id_type=pl.DeviceIdType.MESH)

    def ld_dy(i):
        return pltpu.make_async_copy(dy.at[pl.ds(pl.multiple_of(i * R, R), R)], dyb, insem.at[0])

    def ld_g(i):
        return pltpu.make_async_copy(gate.at[pl.ds(pl.multiple_of(i * R, R), R)], gb, insem.at[1])

    def ld_u(i):
        return pltpu.make_async_copy(up.at[pl.ds(pl.multiple_of(i * R, R), R)], ub, insem.at[2])

    def st(i, k):
        src, dst = ((dgb, dgo), (dub, duo), (hib, hio))[k]
        return pltpu.make_async_copy(src, dst.at[pl.ds(pl.multiple_of(i * R, R), R)], osem.at[k])

    lwd = [pltpu.make_async_copy(wd.at[pl.ds(k * 512, 512)], wdv.at[pl.ds(k * 512, 512)], wsem.at[(0, 3)[k]]) for k in range(2)]
    lw = [None, pltpu.make_async_copy(wg, wgv, wsem.at[1]), pltpu.make_async_copy(wu, wuv, wsem.at[2])]
    ld_dy(0).start()
    lwd[0].start()
    ld_g(0).start()
    ld_u(0).start()
    lwd[1].start()
    lw[1].start()
    lw[2].start()
    if COMM:
        pl.semaphore_wait(bar, 4)

    def phase_a(i, _):
        @pl.when(i > 0)
        def _():
            for k in range(3):
                st(i - 1, k).wait()

        @pl.when(i == 0)
        def _():
            lwd[0].wait()
        ld_dy(i).wait()
        ld_g(i).wait()
        ld_u(i).wait()

        def dblock(j):
            cs = pl.ds(j * 512, 512)
            dh = tb_dot(dyb[...], wdv[cs, :]) if COMP else dyb[:, 0:512].astype(F32)
            g = gb[:, cs].astype(F32)
            u = ub[:, cs].astype(F32)
            s = 1.0 / (1.0 + jnp.exp(-g))
            gs = g * s
            dgb[:, cs] = (dh * u * (s + gs * (1.0 - s))).astype(BF)
            dub[:, cs] = (dh * gs).astype(BF)
            hib[:, cs] = (gs * u).astype(BF)

        dblock(0)
        events(i, 0, 0, NT)

        @pl.when(i == 0)
        def _():
            lwd[1].wait()

        dblock(1)
        for k in range(3):
            st(i, k).start()

        @pl.when(i < NT - 1)
        def _():
            ld_dy(i + 1).start()
            ld_g(i + 1).start()
            ld_u(i + 1).start()

        events(i, 1, 0, NT)

        @pl.when(i == 0)
        def _():
            lw[1].wait()
            lw[2].wait()

        def tblock(j):
            rs_ = pl.ds(pl.multiple_of(j * 512, 512), 512)
            t = tb_dot(dgb[...], wgv[rs_, :]) + tb_dot(dub[...], wuv[rs_, :]) if COMP else dyb[:, rs_].astype(F32)
            for o in range(2):
                a, b = t[2 * o * H:(2 * o + 1) * H], t[(2 * o + 1) * H:(2 * o + 2) * H]
                own[o, :, rs_] = jnp.where(c0, a, b)
                sb0[o, :, rs_] = jnp.where(c0, b, a).astype(BF)

        for p, (lo, hi) in enumerate(((0, 3), (3, 5), (5, 8), (8, 10))):
            pl.loop(lo, hi)(tblock)
            if p == 3 and COMM:
                e_send_core(2 * i)
                e_send_core(2 * i + 1)
            events(i, 2 + p, 0, NT)
        return 0

    lax.fori_loop(0, NT, phase_a, 0)
    for k in range(3):
        st(NT - 1, k).wait()

    dgv, duv = wgv.at[pl.ds(0, N)], wgv.at[pl.ds(N, N)]
    hiv = wuv.at[pl.ds(0, N)]
    K2 = N // 2

    def ld_x(b):
        s = lax.rem(b, 2)
        return pltpu.make_async_copy(x.at[:, pl.ds(pl.multiple_of(b * TB, TB), TB)],
                                     wuv.at[pl.ds(N, N), pl.ds(pl.multiple_of(s * TB, TB), TB)], bsem.at[0, s])

    def ld_dyc(b, h):
        s = lax.rem(b, 2)
        return pltpu.make_async_copy(dy.at[pl.ds(h * K2, K2), pl.ds(pl.multiple_of(b * TB, TB), TB)],
                                     wdv.at[:, pl.ds(pl.multiple_of(s * 2 * TB, TB) + h * TB, TB)], bsem.at[1 + h, s])

    def out_g(b, k):
        s = lax.rem(b, 2)
        v = (wgv, wuv)[k]
        return pltpu.make_async_copy(v.at[pl.ds(pl.multiple_of(2 * N + s * TB, TB), TB)],
                                     (dwg, dwu)[k].at[pl.ds(pl.multiple_of(b * TB, TB), TB)], bout.at[k, s])

    def out_d(b):
        s = lax.rem(b, 2)
        return pltpu.make_async_copy(wdv.at[:, pl.ds(pl.multiple_of(4096 + s * TB, TB), TB)],
                                     dwd.at[:, pl.ds(pl.multiple_of(b * TB, TB), TB)], bout.at[2, s])

    lb = [pltpu.make_async_copy(dgo, dgv, wsem.at[0]), pltpu.make_async_copy(duo, duv, wsem.at[1]), pltpu.make_async_copy(hio, hiv, wsem.at[2])]
    lb[0].start()
    ld_x(0).start()
    lb[1].start()
    if not DOWN2:
        lb[2].start()
        ld_dyc(0, 0).start()
        ld_dyc(0, 1).start()

    def phase_b(b, _):
        t = b + NT
        s = lax.rem(b, 2)

        @pl.when(b < NB - 1)
        def _():
            ld_x(b + 1).start()
            if not DOWN2:
                ld_dyc(b + 1, 0).start()
                ld_dyc(b + 1, 1).start()

        @pl.when(b == 0)
        def _():
            lb[0].wait()
        ld_x(b).wait()
        xs = pl.ds(pl.multiple_of(s * TB, TB), TB)
        for k in range(2):
            @pl.when(b >= 2)
            def _():
                out_g(b - 2, k).wait()

            if k == 1:
                @pl.when(b == 0)
                def _():
                    lb[1].wait()
            r = ta_dot(wuv[pl.ds(N, N), xs], (dgv, duv)[k][...]) if COMP else wuv[0:512, :].astype(F32)
            (wgv, wuv)[k][pl.ds(pl.multiple_of(2 * N + s * TB, TB), TB), :] = r.astype(BF)
            out_g(b, k).start()
            events(t, 2 * k, NT, NT + NB)
            events(t, 2 * k + 1, NT, NT + NB)

        if not DOWN2:
            @pl.when(b >= 2)
            def _():
                out_d(b - 2).wait()

            @pl.when(b == 0)
            def _():
                lb[2].wait()
            ld_dyc(b, 0).wait()
            ld_dyc(b, 1).wait()
            y0 = wdv[:, pl.ds(pl.multiple_of(s * 2 * TB, TB), TB)]
            y1 = wdv[:, pl.ds(pl.multiple_of(s * 2 * TB, TB) + TB, TB)]
            r = ta_dot(hiv[pl.ds(0, K2), :], y0) + ta_dot(hiv[pl.ds(K2, K2), :], y1) if COMP else y0.astype(F32)
            wdv[:, pl.ds(pl.multiple_of(4096 + s * TB, TB), TB)] = r.astype(BF)
            out_d(b).start()
        events(t, 4, NT, NT + NB)
        events(t, 5, NT, NT + NB)
        return 0

    lax.fori_loop(0, NB, phase_b, 0)
    last = NT + max(o for v in OFF.values() for o in v) // PT
    if COMM and last > NT + NB:
        def drain(t, _):
            for p in range(PT):
                events(t, p, NT + NB, last)
            return 0
        lax.fori_loop(NT + NB, last, drain, 0)

    for b in (NB - 2, NB - 1):
        out_g(b, 0).wait()
        out_g(b, 1).wait()
        if not DOWN2:
            out_d(b).wait()
    if COMM:
        def tail(c, _):
            cp("acore", c).wait_recv()
            cp("acore", c).wait_send()
            cp("ap1", c).wait_send()

            @pl.when(inner)
            def _():
                cp("a2", c).wait_send()
                cp("a3", c).wait_send()
            return 0
        lax.fori_loop(0, CH, tail, 0)

        def tail2(c, _):
            cp("p1", c).wait_send()

            @pl.when(inner)
            def _():
                cp("s2", c).wait_send()
                cp("s3", c).wait_send()

            @pl.when(outer)
            def _():
                cp("s1", c).wait_send()
                cp("p3", c).wait_send()
                cp("a1", c).wait_send()
            return 0
        lax.fori_loop(CH - DEP, CH, tail2, 0)


def call(dy, gate, up, wg, wu, wd, x):
    s = jax.ShapeDtypeStruct
    V = pltpu.VMEM
    S = pltpu.SemaphoreType
    any_ = pl.BlockSpec(memory_space=pl.ANY)
    return pl.pallas_call(
        kernel,
        in_specs=[any_] * 7,
        out_specs=[any_] * 7,
        out_shape=[s((N, D), BF), s((D, F), BF), s((D, F), BF), s((F, D), BF), s((N, F), BF), s((N, F), BF), s((N, F), BF)],
        scratch_shapes=[
            V((F, D), BF), V((D, F), BF), V((D, F), BF), V((R, D), BF), V((R, F), BF), V((R, F), BF),
            V((R, F), BF), V((R, F), BF), V((R, F), BF),
            V((2, H, D), F32), V((2, H, D), BF), V((DEP, Q, D), BF), V((KD, Q, D), F32),
            V((DEP, E, D), BF), V((DEP, E, D), BF), V((DEP, E, D), BF), V((DEP, E, D), BF), V((DEP, E, D), BF),
            V((DEP, H, D), BF), V((DEP, Q, D), BF), V((DEP, E, D), BF), V((DEP, E, D), BF), V((DEP, E, D), BF), V((DEP, E, D), BF),
            S.DMA((3,)), S.DMA((4,)), S.DMA((3,)), S.DMA((3, 2)), S.DMA((3, 2)), S.DMA((DEP,)),
            S.DMA((len(NTYPE), CH)), S.DMA((len(NTYPE), CH)), S.REGULAR((6,)),
        ],
        compiler_params=pltpu.CompilerParams(collective_id=0, has_side_effects=True, vmem_limit_bytes=67043328) if COMM
        else pltpu.CompilerParams(vmem_limit_bytes=67043328),
        cost_estimate=pl.CostEstimate(flops=6 * 2 * N * D * F, bytes_accessed=200 * 2**20, transcendentals=N * F),
        name="mlp_bwd",
    )(dy, gate, up, wg, wu, wd, x)


def finish_kernel(hi, dy, dx, dwg, dwu, dwd, odx, odwg, odwu, odwd):
    odx[...] = dx[...]
    odwg[...] = dwg[...]
    odwu[...] = dwu[...]
    if DOWN2:
        odwd[...] = ta_dot(hi[...], dy[...]).astype(BF)
    else:
        odwd[...] = dwd[...]


def finish(hi, dy, dx, dwg, dwu, dwd):
    s = jax.ShapeDtypeStruct
    col = lambda n: pl.BlockSpec((n, TB), lambda j: (0, j))
    row = pl.BlockSpec((TB, F), lambda j: (j, 0))
    any_ = pl.BlockSpec(memory_space=pl.ANY)
    return pl.pallas_call(
        finish_kernel,
        grid=(NB,),
        in_specs=[pl.BlockSpec((N, F), lambda j: (0, 0)) if DOWN2 else any_, col(N) if DOWN2 else any_, col(N), row, row, any_ if DOWN2 else col(F)],
        out_specs=[col(N), row, row, col(F)],
        out_shape=[s((N, D), BF), s((D, F), BF), s((D, F), BF), s((F, D), BF)],
        compiler_params=pltpu.CompilerParams(vmem_limit_bytes=60 * 2**20),
        cost_estimate=pl.CostEstimate(flops=2 * N * D * F, bytes_accessed=118 * 2**20, transcendentals=0),
        name="finish",
    )(hi, dy, dx, dwg, dwu, dwd)


def solution(mesh):
    def step(x, dy, gate, up, w_gate, w_up, w_down):
        dx, dwg, dwu, dwd, _, _, hi = call(dy, gate, up, w_gate, w_up, w_down, x)
        return finish(hi, dy, dx, dwg, dwu, dwd)

    tokens, columns, rows = P("dp", None), P(None, "tp"), P("tp", None)
    return jax.shard_map(
        step,
        mesh=mesh,
        in_specs=(tokens, tokens, P("dp", "tp"), P("dp", "tp"), columns, columns, rows),
        out_specs=(tokens, P("dp", "tp"), P("dp", "tp"), P(("dp", "tp"), None)),
        check_vma=False,
    )
```
